512 devices in a mesh: gx: 64 (over x, y, core), ta: 8 (over z).
Axes of the slice: x: 4, y: 8, z: 8, core: 2. Of those that a mesh axis runs over, the one named last changes fastest.
Arguments:
- master_flat: float32 [8388608], P(('gx', 'ta')), may hold values from -6 to 6
Outputs:
- serving_weight: bfloat16 [1, 8192, 1024], P(None, None, 'ta')
- channel_scale: float32 [1, 1024], P(None, 'ta')
The draws below stay inside these ranges and needn't reach their ends.
All inputs are finite; a program needn't handle non-finite values.
Results may differ from the reference program's by a relative error of at most 0.015.
Values may be sent and summed in bfloat16 or wider, within the bound.
No kernel may reach another device: no remote copies, remote signals or barrier semaphores. Data moves between devices by JAX's collectives and lax.ppermute only.
A program may use at most 64 MiB of HBM per device.

```python
import jax
import jax.numpy as jnp

D = 8192
KVH = 8
HEAD = 128
LAYERS = 1


def level_of(own_key, dims, split, least, top_value):
    factor_of, own = 1.0, jax.random.fold_in(own_key, 6)
    for axis_at, blocks in split:
        steps = jnp.exp(jax.random.uniform(jax.random.fold_in(own, axis_at), (blocks,), jnp.float32, least / len(split), top_value / len(split)))
        factor_of = factor_of * jnp.repeat(steps, dims[axis_at] // blocks).reshape([-1 if axis == axis_at else 1 for axis in range(len(dims))])
    return factor_of


def gaussian(key, shape, deviation, bound, cuts=(), kind=jnp.bfloat16):
    level = level_of(key, shape, cuts, -0.22, 0.18) if cuts else 1.0
    values = jax.random.normal(key, shape, jnp.float32) * deviation * level
    return jnp.minimum(jnp.maximum(values, -bound), bound).astype(kind)


def setup_inputs(seed: int = 0) -> dict:
    seeds = jax.random.split(jax.random.key(seed), 2)
    return {
        "master_flat": gaussian(seeds[0], (LAYERS * D * KVH * HEAD,), 1.0, 6.0, ((0, 512),), jnp.float32),
    }


def reference(master_flat):
    weight = master_flat.reshape(LAYERS, D, KVH * HEAD).astype(jnp.bfloat16)
    wide = weight.astype(jnp.float32)
    channel_scale = jnp.max(jnp.abs(wide), axis=1)
    serving_weight = (wide / channel_scale[:, None, :]).astype(jnp.bfloat16)
    return serving_weight, channel_scale
```

```python
import jax
import jax.numpy as jnp
from jax import lax
from jax.sharding import Mesh, PartitionSpec as P

D = 8192
KVH = 8
HEAD = 128
LAYERS = 1
AXES = ("x", "yh", "yl", "c", "ta")


def exchange(block, peers, axes):
    copies = jnp.broadcast_to(block[None], (peers,) + block.shape)
    return lax.all_to_all(copies, axes, 0, 0, tiled=True)


def shards(master_flat):
    rounded = master_flat.astype(jnp.bfloat16).reshape(16, 8, 128)
    by_channel = jnp.transpose(rounded, (1, 0, 2))
    copies = jnp.broadcast_to(by_channel[None], (4, 8, 16, 128)).reshape(32, 16, 128)
    part = lax.all_to_all(copies, ("yh", "ta"), 0, 0, tiled=True).reshape(512, 128)
    plane = exchange(part, 8, ("x", "yl")).reshape(4, 2, 4, 128, 128)
    own = jnp.transpose(plane, (0, 2, 1, 3, 4)).reshape(32, 128, 128)
    other = lax.ppermute(own, "c", [(0, 1), (1, 0)])
    core = lax.axis_index("c")
    top = jnp.maximum(jnp.max(jnp.abs(own), axis=(0, 1)), jnp.max(jnp.abs(other), axis=(0, 1)))
    channel_scale = top.astype(jnp.float32)
    first = jnp.where(core == 0, own, other)
    second = jnp.where(core == 0, other, own)
    weight = jnp.stack([first, second], 1).astype(jnp.float32)
    serving_weight = (weight / channel_scale).astype(jnp.bfloat16)
    return serving_weight.reshape(LAYERS, D, HEAD), channel_scale[None]


def solution(mesh):
    fine = Mesh(mesh.devices.reshape(4, 4, 2, 2, 8), AXES)
    out_specs = (P(None, None, "ta"), P(None, "ta"))
    return jax.shard_map(shards, mesh=fine, in_specs=(P(AXES),), out_specs=out_specs, check_vma=False)
```

```python
import jax
import jax.numpy as jnp
from jax import lax
from jax.experimental import pallas as pl
from jax.experimental.pallas import tpu as pltpu
from jax.sharding import Mesh, PartitionSpec as P

D = 8192
KVH = 8
HEAD = 128
LAYERS = 1
X, Y, C, Z = 4, 8, 2, 8
AXES = ("x", "y", "c", "ta")
ROWS = 128


def device(x, y, c, z):
    return (((x % X) * Y + y % Y) * C + c) * Z + z


def far_groups():
    return [
        [device(x, 2 * yh + yp, c, z) for yh in range(Y // 2) for z in range(Z)]
        for x in range(X) for yp in range(2) for c in range(C)
    ]


def near_groups():
    return [
        [device(x, y, c, z) for x in range(X) for y in (2 * j, 2 * j + 1)]
        for c in range(C) for z in range(Z) for j in range(Y // 2)
    ]


def exchange(blocks, groups):
    return lax.all_to_all(blocks, AXES, 0, 0, axis_index_groups=groups, tiled=True)


CHUNKS = 8


def finish_kernel(top_ref, own_ref, other_ref, out_ref, scale_ref, stage_ref, row_ref, sems):
    core = lax.axis_index("c")
    top = jnp.maximum(top_ref[...], jnp.max(jnp.abs(other_ref[...]).reshape(-1, 16, HEAD), axis=0).max(axis=0, keepdims=True))
    scale = top.astype(jnp.float32)
    row_ref[...] = scale
    factor = 1.0 / scale
    copies = [pltpu.make_async_copy(row_ref, scale_ref, sems.at[CHUNKS])]
    copies[0].start()
    for k in range(CHUNKS):
        x, part = divmod(k, 2)
        for yh in (2 * part, 2 * part + 1):
            for yp in range(2):
                source = (x * 2 + yp) * 4 + yh
                target = (x * 4 + yh) * 2 + yp
                stage_ref[target, core] = (own_ref[source].astype(jnp.float32) * factor).astype(jnp.bfloat16)
                stage_ref[target, 1 - core] = (other_ref[source].astype(jnp.float32) * factor).astype(jnp.bfloat16)
        copy = pltpu.make_async_copy(stage_ref.at[pl.ds(4 * k, 4)], out_ref.at[pl.ds(4 * k, 4)], sems.at[k])
        copy.start()
        copies.append(copy)
    for copy in copies:
        copy.wait()


def finish(top, own, other):
    vmem = pl.BlockSpec(memory_space=pltpu.VMEM)
    return pl.pallas_call(
        finish_kernel,
        in_specs=[vmem, vmem, vmem],
        out_specs=[pl.BlockSpec(memory_space=pl.ANY), pl.BlockSpec(memory_space=pl.ANY)],
        out_shape=[
            jax.ShapeDtypeStruct((32, 2, ROWS, HEAD), jnp.bfloat16),
            jax.ShapeDtypeStruct((1, HEAD), jnp.float32),
        ],
        scratch_shapes=[
            pltpu.VMEM((32, 2, ROWS, HEAD), jnp.bfloat16),
            pltpu.VMEM((1, HEAD), jnp.float32),
            pltpu.SemaphoreType.DMA((CHUNKS + 1,)),
        ],
        name="finish",
    )(*(pltpu.with_memory_space_constraint(part, pltpu.VMEM) for part in (top, own, other)))


def shards(master_flat):
    rounded = master_flat.astype(jnp.bfloat16).reshape(16, 8, HEAD)
    by_channel = jnp.transpose(rounded, (1, 0, 2))
    copies = jnp.broadcast_to(by_channel[None], (4, 8, 16, HEAD)).reshape(32, 16, HEAD)
    far = exchange(copies, far_groups()).reshape(512, HEAD)
    copies = jnp.broadcast_to(far[None], (8, 512, HEAD))
    own = exchange(copies, near_groups()).reshape(32, ROWS, HEAD)
    other = lax.ppermute(own, "c", [(0, 1), (1, 0)])
    top = jnp.max(jnp.abs(own), axis=(0, 1))[None]
    weight, channel_scale = finish(top, own, other)
    return weight.reshape(LAYERS, D, HEAD), channel_scale


def solution(mesh):
    fine = Mesh(mesh.devices.reshape(X, Y, C, Z), AXES)
    out_specs = (P(None, None, "ta"), P(None, "ta"))
    return jax.shard_map(shards, mesh=fine, in_specs=(P(AXES),), out_specs=out_specs, check_vma=False)
```

```python
import jax
import jax.numpy as jnp
from jax import lax
from jax.experimental import pallas as pl
from jax.experimental.pallas import tpu as pltpu
from jax.sharding import Mesh, PartitionSpec as P

D = 8192
KVH = 8
HEAD = 128
LAYERS = 1
X, Y, C, Z = 4, 8, 2, 8
AXES = ("x", "y", "c", "ta")
ROWS = 128


def device(x, y, c, z):
    return (((x % X) * Y + y % Y) * C + c) * Z + z


def far_groups():
    return [
        [device(x, 2 * yh + yp, c, 2 * zh + zp) for yh in range(Y // 2) for zh in range(Z // 2)]
        for x in range(X) for yp in range(2) for c in range(C) for zp in range(2)
    ]


def pairs(size, c):
    return [(2 * i, (2 * i + 1 - 2 * c) % size) for i in range(size // 2)]


def near_groups():
    return [
        [device(x, y, c, z) for x in range(X) for y in ys for z in zs]
        for c in range(C) for ys in pairs(Y, c) for zs in pairs(Z, c)
    ]


def exchange(blocks, groups):
    return lax.all_to_all(blocks, AXES, 0, 0, axis_index_groups=groups, tiled=True)


CHUNKS = 8


def finish_kernel(top_ref, own_ref, other_ref, out_ref, scale_ref, stage_ref, row_ref, sems):
    core = lax.axis_index("c")
    top = jnp.maximum(top_ref[...], jnp.max(jnp.abs(other_ref[...]).reshape(-1, 16, HEAD), axis=0).max(axis=0, keepdims=True))
    scale = top.astype(jnp.float32)
    row_ref[...] = scale
    factor = 1.0 / scale
    copies = [pltpu.make_async_copy(row_ref, scale_ref, sems.at[CHUNKS])]
    copies[0].start()
    for k in range(CHUNKS):
        x, part = divmod(k, 2)
        for yh in (2 * part, 2 * part + 1):
            for yp in range(2):
                target = (x * 4 + yh) * 2 + yp
                for zp in range(2):
                    source = ((x * 2 + yp) * 2 + zp) * 4 + yh
                    stage_ref[target, core, :, zp] = (own_ref[source].astype(jnp.float32) * factor).astype(jnp.bfloat16)
                    stage_ref[target, 1 - core, :, zp] = (other_ref[source].astype(jnp.float32) * factor).astype(jnp.bfloat16)
        copy = pltpu.make_async_copy(stage_ref.at[pl.ds(4 * k, 4)], out_ref.at[pl.ds(4 * k, 4)], sems.at[k])
        copy.start()
        copies.append(copy)
    for copy in copies:
        copy.wait()


def finish(top, own, other):
    vmem = pl.BlockSpec(memory_space=pltpu.VMEM)
    return pl.pallas_call(
        finish_kernel,
        in_specs=[vmem, vmem, vmem],
        out_specs=[pl.BlockSpec(memory_space=pl.ANY), pl.BlockSpec(memory_space=pl.ANY)],
        out_shape=[
            jax.ShapeDtypeStruct((32, 2, Z // 2, 2, 16, HEAD), jnp.bfloat16),
            jax.ShapeDtypeStruct((1, HEAD), jnp.float32),
        ],
        scratch_shapes=[
            pltpu.VMEM((32, 2, Z // 2, 2, 16, HEAD), jnp.bfloat16),
            pltpu.VMEM((1, HEAD), jnp.float32),
            pltpu.SemaphoreType.DMA((CHUNKS + 1,)),
        ],
        name="finish",
    )(*(pltpu.with_memory_space_constraint(part, pltpu.VMEM) for part in (top, own, other)))


def shards(master_flat):
    rounded = master_flat.astype(jnp.bfloat16).reshape(16, 8, HEAD)
    by_channel = jnp.transpose(rounded, (1, 0, 2))
    even, odd = by_channel[0::2], by_channel[1::2]
    second_core, odd_plane = lax.axis_index("c") == 1, lax.axis_index("ta") % 2 == 1
    even = jnp.where(second_core & odd_plane, jnp.roll(even, -1, 0), even)
    odd = jnp.where(second_core & ~odd_plane, jnp.roll(odd, 1, 0), odd)
    by_pair = jnp.stack([even, odd], 1)
    copies = jnp.broadcast_to(by_pair[None], (4, 4, 2, 16, HEAD)).reshape(16, 2, 16, HEAD)
    far = exchange(copies, far_groups())
    far = jnp.transpose(far, (1, 0, 2, 3))
    copies = jnp.broadcast_to(far[None], (8, 2, 16, 16, HEAD)).reshape(16, 16, 16, HEAD)
    own = exchange(copies, near_groups()).reshape(64, 4, 16, HEAD)
    other = lax.ppermute(own, "c", [(0, 1), (1, 0)])
    top = jnp.max(jnp.abs(own), axis=(0, 1, 2))[None]
    weight, channel_scale = finish(top, own, other)
    return weight.reshape(LAYERS, D, HEAD), channel_scale


def solution(mesh):
    fine = Mesh(mesh.devices.reshape(X, Y, C, Z), AXES)
    out_specs = (P(None, None, "ta"), P(None, "ta"))
    return jax.shard_map(shards, mesh=fine, in_specs=(P(AXES),), out_specs=out_specs, check_vma=False)
```

```python
import jax
import jax.numpy as jnp
from jax import lax
from jax.experimental import pallas as pl
from jax.experimental.pallas import tpu as pltpu
from jax.sharding import Mesh, PartitionSpec as P

D = 8192
KVH = 8
HEAD = 128
LAYERS = 1
X, Y, C, Z = 4, 8, 2, 8
AXES = ("x", "y", "c", "ta")
ROWS = 128


def device(x, y, c, z):
    return (((x % X) * Y + y % Y) * C + c) * Z + z


def far_groups():
    return [
        [device(x, 2 * yh + yp, c, 2 * zh + zp) for yh in range(Y // 2) for zh in range(Z // 2)]
        for x in range(X) for yp in range(2) for c in range(C) for zp in range(2)
    ]


def pairs(size, c):
    return [(2 * i, (2 * i + 1 - 2 * c) % size) for i in range(size // 2)]


def near_groups():
    return [
        [device(x, y, c, z) for x in range(X) for y in ys for z in zs]
        for c in range(C) for ys in pairs(Y, c) for zs in pairs(Z, 0)
    ]


def exchange(blocks, groups):
    return lax.all_to_all(blocks, AXES, 0, 0, axis_index_groups=groups, tiled=True)


CHUNKS = 8


def finish_kernel(top_ref, own_ref, other_ref, out_ref, scale_ref, stage_ref, row_ref, sems):
    core = lax.axis_index("c")
    top = jnp.maximum(top_ref[...], jnp.max(jnp.abs(other_ref[...]).reshape(-1, 16, HEAD), axis=0).max(axis=0, keepdims=True))
    scale = top.astype(jnp.float32)
    row_ref[...] = scale
    factor = 1.0 / scale
    copies = [pltpu.make_async_copy(row_ref, scale_ref, sems.at[CHUNKS])]
    copies[0].start()
    for k in range(CHUNKS):
        x, part = divmod(k, 2)
        for yh in (2 * part, 2 * part + 1):
            for yp in range(2):
                target = (x * 4 + yh) * 2 + yp
                for zp in range(2):
                    source = ((x * 2 + yp) * 2 + zp) * 4 + yh
                    stage_ref[target, core, :, zp] = (own_ref[source].astype(jnp.float32) * factor).astype(jnp.bfloat16)
                    stage_ref[target, 1 - core, :, zp] = (other_ref[source].astype(jnp.float32) * factor).astype(jnp.bfloat16)
        copy = pltpu.make_async_copy(stage_ref.at[pl.ds(4 * k, 4)], out_ref.at[pl.ds(4 * k, 4)], sems.at[k])
        copy.start()
        copies.append(copy)
    for copy in copies:
        copy.wait()


def finish(top, own, other):
    vmem = pl.BlockSpec(memory_space=pltpu.VMEM)
    return pl.pallas_call(
        finish_kernel,
        in_specs=[vmem, vmem, vmem],
        out_specs=[pl.BlockSpec(memory_space=pl.ANY), pl.BlockSpec(memory_space=pl.ANY)],
        out_shape=[
            jax.ShapeDtypeStruct((32, 2, Z // 2, 2, 16, HEAD), jnp.bfloat16),
            jax.ShapeDtypeStruct((1, HEAD), jnp.float32),
        ],
        scratch_shapes=[
            pltpu.VMEM((32, 2, Z // 2, 2, 16, HEAD), jnp.bfloat16),
            pltpu.VMEM((1, HEAD), jnp.float32),
            pltpu.SemaphoreType.DMA((CHUNKS + 1,)),
        ],
        name="finish",
    )(*(pltpu.with_memory_space_constraint(part, pltpu.VMEM) for part in (top, own, other)))


def shards(master_flat):
    rounded = master_flat.astype(jnp.bfloat16).reshape(16, 8, HEAD)
    by_channel = jnp.transpose(rounded, (1, 0, 2))
    by_pair = by_channel.reshape(4, 2, 16, HEAD)
    copies = jnp.broadcast_to(by_pair[None], (4, 4, 2, 16, HEAD)).reshape(16, 2, 16, HEAD)
    far = exchange(copies, far_groups())
    far = jnp.transpose(far, (1, 0, 2, 3))
    copies = jnp.broadcast_to(far[None], (8, 2, 16, 16, HEAD)).reshape(16, 16, 16, HEAD)
    own = exchange(copies, near_groups()).reshape(64, 4, 16, HEAD)
    other = lax.ppermute(own, "c", [(0, 1), (1, 0)])
    top = jnp.max(jnp.abs(own), axis=(0, 1, 2))[None]
    weight, channel_scale = finish(top, own, other)
    return weight.reshape(LAYERS, D, HEAD), channel_scale


def solution(mesh):
    fine = Mesh(mesh.devices.reshape(X, Y, C, Z), AXES)
    out_specs = (P(None, None, "ta"), P(None, "ta"))
    return jax.shard_map(shards, mesh=fine, in_specs=(P(AXES),), out_specs=out_specs, check_vma=False)
```

```python
import jax
import jax.numpy as jnp
from jax import lax
from jax.experimental import pallas as pl
from jax.experimental.pallas import tpu as pltpu
from jax.sharding import Mesh, PartitionSpec as P

D = 8192
KVH = 8
HEAD = 128
LAYERS = 1
X, Y, C, Z = 4, 8, 2, 8
AXES = ("x", "y", "c", "ta")
ROWS = 128


def device(x, y, c, z):
    return (((x % X) * Y + y % Y) * C + c) * Z + z


def far_groups():
    return [
        [device(x, 2 * yh + yp, c, 2 * zh + zp) for yh in range(Y // 2) for zh in range(Z // 2)]
        for x in range(X) for yp in range(2) for c in range(C) for zp in range(2)
    ]


def pairs(size, c):
    return [(2 * i, (2 * i + 1 - 2 * c) % size) for i in range(size // 2)]


def near_groups():
    return [
        [device(x, y, c, z) for x in range(X) for y in ys for z in zs]
        for c in range(C) for ys in pairs(Y, c) for zs in pairs(Z, c)
    ]


def exchange(blocks, groups):
    return lax.all_to_all(blocks, AXES, 0, 0, axis_index_groups=groups, tiled=True)


CHUNKS = 8


def finish_kernel(top_ref, own_ref, other_ref, out_ref, scale_ref, stage_ref, row_ref, sems):
    core = lax.axis_index("c")
    top = jnp.maximum(top_ref[...], jnp.max(jnp.abs(other_ref[...]).reshape(-1, 16, HEAD), axis=0).max(axis=0, keepdims=True))
    scale = top.astype(jnp.float32)
    row_ref[...] = scale
    factor = 1.0 / scale
    copies = [pltpu.make_async_copy(row_ref, scale_ref, sems.at[CHUNKS])]
    copies[0].start()
    for k in range(CHUNKS):
        x, part = divmod(k, 2)
        for yh in (2 * part, 2 * part + 1):
            for yp in range(2):
                target = (x * 4 + yh) * 2 + yp
                for zp in range(2):
                    source = ((x * 2 + yp) * 2 + zp) * 4 + yh
                    stage_ref[target, core, :, zp] = (own_ref[source].astype(jnp.float32) * factor).astype(jnp.bfloat16)
                    stage_ref[target, 1 - core, :, zp] = (other_ref[source].astype(jnp.float32) * factor).astype(jnp.bfloat16)
        copy = pltpu.make_async_copy(stage_ref.at[pl.ds(4 * k, 4)], out_ref.at[pl.ds(4 * k, 4)], sems.at[k])
        copy.start()
        copies.append(copy)
    for copy in copies:
        copy.wait()


def finish(top, own, other):
    vmem = pl.BlockSpec(memory_space=pltpu.VMEM)
    return pl.pallas_call(
        finish_kernel,
        in_specs=[vmem, vmem, vmem],
        out_specs=[pl.BlockSpec(memory_space=pl.ANY), pl.BlockSpec(memory_space=pl.ANY)],
        out_shape=[
            jax.ShapeDtypeStruct((32, 2, Z // 2, 2, 16, HEAD), jnp.bfloat16),
            jax.ShapeDtypeStruct((1, HEAD), jnp.float32),
        ],
        scratch_shapes=[
            pltpu.VMEM((32, 2, Z // 2, 2, 16, HEAD), jnp.bfloat16),
            pltpu.VMEM((1, HEAD), jnp.float32),
            pltpu.SemaphoreType.DMA((CHUNKS + 1,)),
        ],
        name="finish",
    )(*(pltpu.with_memory_space_constraint(part, pltpu.VMEM) for part in (top, own, other)))


def spread_kernel(flat_ref, out_ref):
    second_core, odd_plane = lax.axis_index("c"), lax.axis_index("ta") % 2
    for zh in range(Z // 2):
        even = (2 * zh + 2 * second_core * odd_plane) % Z
        odd = (2 * zh + 1 + (Z - 2) * second_core * (1 - odd_plane)) % Z
        for zl, channel in enumerate((even, odd)):
            block = flat_ref[pl.ds(channel, 16, stride=Z), :].astype(jnp.bfloat16)
            for yh in range(Y // 2):
                out_ref[yh * 4 + zh, zl] = block


def spread(flat):
    vmem = pl.BlockSpec(memory_space=pltpu.VMEM)
    return pl.pallas_call(
        spread_kernel,
        in_specs=[vmem],
        out_specs=vmem,
        out_shape=pltpu.VMEM((16, 2, 16, HEAD), jnp.bfloat16),
        name="spread",
    )(flat)


def shards(master_flat):
    copies = spread(master_flat.reshape(16 * Z, HEAD))
    far = exchange(copies, far_groups())
    far = jnp.transpose(far, (1, 0, 2, 3))
    copies = jnp.broadcast_to(far[None], (8, 2, 16, 16, HEAD)).reshape(16, 16, 16, HEAD)
    own = exchange(copies, near_groups()).reshape(64, 4, 16, HEAD)
    other = lax.ppermute(own, "c", [(0, 1), (1, 0)])
    top = jnp.max(jnp.abs(own), axis=(0, 1, 2))[None]
    weight, channel_scale = finish(top, own, other)
    return weight.reshape(LAYERS, D, HEAD), channel_scale


def solution(mesh):
    fine = Mesh(mesh.devices.reshape(X, Y, C, Z), AXES)
    out_specs = (P(None, None, "ta"), P(None, "ta"))
    return jax.shard_map(shards, mesh=fine, in_specs=(P(AXES),), out_specs=out_specs, check_vma=False)
```
